1024 devices in a mesh: pipe: 4 (over y_hi), dp: 32 (over y_lo, z), tensor: 8 (over x, core).
Axes of the slice: x: 4, y: 8 (y_hi: 4, y_lo: 2; y = y_hi * 2 + y_lo), z: 16, core: 2. Of those that a mesh axis runs over, the one named last changes fastest.
Arguments:
- saved: bfloat16 [4, 2, 2048, 1024], P('pipe', None, 'dp'), may hold values from -6 to 6
- top_grad: bfloat16 [2, 2048, 1024], P(None, 'dp'), may hold values from -6 to 6
- gain: bfloat16 [4, 1024], P('pipe', 'dp'), may hold values from 0.25 to 1.75
- w_query: bfloat16 [4, 1024, 1536], P('pipe', 'dp', 'tensor'), may hold values from -0.1875 to 0.1875
- w_latent: bfloat16 [4, 1024, 576], P('pipe', 'dp'), may hold values from -0.1875 to 0.1875
- compressed_gain: bfloat16 [4, 512], P('pipe', 'dp'), may hold values from 0.25 to 1.75
- expand_weight: bfloat16 [4, 512, 2048], P('pipe', 'dp', 'tensor'), may hold values from -0.25 to 0.25
- w_output: bfloat16 [4, 1024, 1024], P('pipe', 'tensor', 'dp'), may hold values from -0.1875 to 0.1875
Outputs:
- input_grad: bfloat16 [4, 2, 2048, 1024], P('pipe', None, ('dp', 'tensor'))
- grad_gain: float32 [4, 1024], P('pipe', 'dp')
- grad_query: float32 [4, 1024, 1536], P('pipe', 'dp', 'tensor')
- grad_latent: float32 [4, 1024, 576], P('pipe', 'dp')
- grad_latent_gain: float32 [4, 512], P('pipe', 'dp')
- grad_expand: float32 [4, 512, 2048], P('pipe', 'dp', 'tensor')
- grad_output: float32 [4, 1024, 1024], P('pipe', 'tensor', 'dp')
The draws below stay inside these ranges and needn't reach their ends.
All inputs are finite; a program needn't handle non-finite values.
Results may differ from the reference program's by a relative error of at most 0.04.
Values may be sent and summed in bfloat16 or wider, within the bound.
A program may use at most 64 MiB of HBM per device.

```python
import jax
import jax.numpy as jnp
from jax import lax

MODEL_WIDTH = 1024
NOPE = 128
ROPE = 64
VDIM = 128
COMPRESSED_RANK = 512
MB = 2
MB_TOK = 64
SECTION_COUNT = 4
TOKENS = 2048
QUERY_COLUMNS = 1536
LATENT_COLUMNS = 576
EXPAND_COLUMNS = 2048
OUTPUT_ROWS = 1024
N_DP = 32
N_TENSOR = 8


def steps_of(rng, dims, pieces, low, top_value):
    def one(position, blocks):
        heights = jax.random.uniform(jax.random.fold_in(jax.random.fold_in(rng, 6), position), (blocks,), jnp.float32, low / len(pieces), top_value / len(pieces))
        return jnp.repeat(jnp.exp(heights), dims[position] // blocks).reshape((-1,) + (1,) * (len(dims) - position - 1))

    level = one(*pieces[0])
    for cut in pieces[1:]:
        level = level * one(*cut)
    return level


def normal_values(rng, dims, deviation, bound, shards=(), kind=jnp.bfloat16):
    array = jax.random.normal(rng, dims, jnp.float32) * deviation
    if len(shards) > 0:
        array = steps_of(rng, dims, shards, -0.22, 0.18) * array
    return jnp.clip(array, min=-bound, max=bound).astype(kind)


def setup_inputs(seed: int = 0) -> dict:
    seeds = jax.random.split(jax.random.key(seed), 9)
    return {
        "saved": normal_values(seeds[0], (SECTION_COUNT, MB, TOKENS, MODEL_WIDTH), 1.0, 6.0, ((0, 4), (2, 32))),
        "top_grad": normal_values(seeds[1], (MB, TOKENS, MODEL_WIDTH), 1.0, 6.0, ((1, 32),)),
        "gain": jnp.clip(1.0 + 0.15 * jax.random.normal(seeds[2], (SECTION_COUNT, MODEL_WIDTH), jnp.float32), 0.25, 1.75).astype(jnp.bfloat16),
        "w_query": normal_values(seeds[3], (SECTION_COUNT, MODEL_WIDTH, QUERY_COLUMNS), MODEL_WIDTH ** -0.5, 0.1875, ((0, 4), (1, 32), (2, 8))),
        "w_latent": normal_values(seeds[4], (SECTION_COUNT, MODEL_WIDTH, LATENT_COLUMNS), MODEL_WIDTH ** -0.5, 0.1875, ((0, 4), (1, 32))),
        "compressed_gain": jnp.clip(1.0 + 0.15 * jax.random.normal(seeds[5], (SECTION_COUNT, COMPRESSED_RANK), jnp.float32), 0.25, 1.75).astype(jnp.bfloat16),
        "expand_weight": normal_values(seeds[6], (SECTION_COUNT, COMPRESSED_RANK, EXPAND_COLUMNS), COMPRESSED_RANK ** -0.5, 0.25, ((0, 4), (1, 32), (2, 8))),
        "w_output": normal_values(seeds[7], (SECTION_COUNT, OUTPUT_ROWS, MODEL_WIDTH), OUTPUT_ROWS ** -0.5, 0.1875, ((0, 4), (1, 8), (2, 32))),
    }


EPS = 1e-06

def root_mean_scale(values, scale):
    return values * lax.rsqrt(lax.optimization_barrier(jnp.mean(values * values, axis=-1, keepdims=True)) + EPS) * scale

def rotary_angles(values):
    length = values.shape[0]
    half = values.shape[-1] // 2
    freq = jnp.exp(-jnp.log(10000.0) * jnp.arange(half, dtype=jnp.float32) / half)
    angle = jnp.arange(length, dtype=jnp.float32)[:, None] * freq[None, :]
    cosine = jnp.cos(angle)[:, None, :]
    sine = jnp.sin(angle)[:, None, :]
    first = values[..., :half]
    second = values[..., half:]
    return jnp.concatenate([first * cosine - second * sine, second * cosine + first * sine], axis=-1)

def branch(normed, w_q, w_lat, latent_norm_gain, w_exp, w_out):
    length = normed.shape[0]
    heads = w_q.shape[1] // (NOPE + ROPE)
    rounded = normed.astype(jnp.bfloat16)
    query = jnp.dot(rounded, w_q, preferred_element_type=jnp.float32).reshape(length, heads, NOPE + ROPE)
    latent_state = jnp.dot(rounded, w_lat, preferred_element_type=jnp.float32)
    compressed_state = root_mean_scale(latent_state[:, :COMPRESSED_RANK], latent_norm_gain).astype(jnp.bfloat16)
    rotary_key_part = rotary_angles(latent_state[:, None, COMPRESSED_RANK:])[:, 0, :]
    expanded = jnp.dot(compressed_state, w_exp, preferred_element_type=jnp.float32).reshape(length, heads, NOPE + VDIM)
    key_nope = expanded[:, :, :NOPE]
    values = expanded[:, :, NOPE:].astype(jnp.bfloat16)
    query_rope = rotary_angles(query[:, :, NOPE:])
    scores = jnp.einsum('qhd,khd->hqk', query[:, :, :NOPE], key_nope) + jnp.einsum('qhd,kd->hqk', query_rope, rotary_key_part)
    scores = scores * (NOPE + ROPE) ** (-0.5)
    causal = jnp.arange(length)[:, None] >= jnp.arange(length)[None, :]
    scores = jnp.where(causal[None], scores, -1e+30)
    weights = jax.nn.softmax(scores, axis=-1).astype(jnp.bfloat16)
    mixed = jnp.einsum('hqk,khd->qhd', weights.astype(jnp.float32), values.astype(jnp.float32))
    mixed = mixed.astype(jnp.bfloat16).reshape(length, heads * VDIM)
    return jnp.dot(mixed, w_out, preferred_element_type=jnp.float32)

def reference(saved, top_grad, gain, w_query, w_latent, compressed_gain, expand_weight, w_output):
    head_groups = N_TENSOR
    dgrads = []
    all_input = []
    upstream = top_grad
    for section_index in reversed(range(SECTION_COUNT)):
        gain32 = gain[section_index].astype(jnp.float32)
        lgain32 = compressed_gain[section_index].astype(jnp.float32)
        lat_w = w_latent[section_index]
        q_groups = w_query[section_index].reshape(MODEL_WIDTH, head_groups, QUERY_COLUMNS // head_groups).transpose(1, 0, 2)
        expand_groups = expand_weight[section_index].reshape(COMPRESSED_RANK, head_groups, EXPAND_COLUMNS // head_groups).transpose(1, 0, 2)
        o_groups = w_output[section_index].reshape(head_groups, OUTPUT_ROWS // head_groups, MODEL_WIDTH)

        def one_sequence(loop_carry, pair):
            x_rows, up_rows = pair
            normed, norm_pull = jax.vjp(root_mean_scale, x_rows.astype(jnp.float32), gain32)
            cot = up_rows.astype(jnp.float32)

            def one_group(wq_g, we_g, wo_g):
                unused, pull = jax.vjp(branch, normed, wq_g, lat_w, lgain32, we_g, wo_g)
                return pull(cot)
            d_norm, d_q, d_lat, d_lg, expand_gradient, d_o = jax.vmap(one_group)(q_groups, expand_groups, o_groups)
            d_normed = lax.optimization_barrier(jnp.sum(d_norm, axis=0))
            dx_norm, d_gain = norm_pull(d_normed)
            dx = (cot + dx_norm).astype(jnp.bfloat16)
            g_q = d_q.astype(jnp.float32).transpose(1, 0, 2).reshape(MODEL_WIDTH, QUERY_COLUMNS)
            expand_weight_grad = expand_gradient.astype(jnp.float32).transpose(1, 0, 2).reshape(COMPRESSED_RANK, EXPAND_COLUMNS)
            g_o = d_o.astype(jnp.float32).reshape(OUTPUT_ROWS, MODEL_WIDTH)
            g_lat = lax.optimization_barrier(jnp.sum(d_lat.astype(jnp.float32), axis=0))
            g_lg = lax.optimization_barrier(jnp.sum(d_lg, axis=0))
            loop_carry = (loop_carry[0] + d_gain, loop_carry[1] + g_q, loop_carry[2] + g_lat, loop_carry[3] + g_lg, loop_carry[4] + expand_weight_grad, loop_carry[5] + g_o)
            return (loop_carry, dx)
        loop_carry = (jnp.zeros((MODEL_WIDTH,), jnp.float32), jnp.zeros((MODEL_WIDTH, QUERY_COLUMNS), jnp.float32), jnp.zeros((MODEL_WIDTH, LATENT_COLUMNS), jnp.float32), jnp.zeros((COMPRESSED_RANK,), jnp.float32), jnp.zeros((COMPRESSED_RANK, EXPAND_COLUMNS), jnp.float32), jnp.zeros((OUTPUT_ROWS, MODEL_WIDTH), jnp.float32))
        section_inputs = []
        for micro in range(MB):
            x_seq = saved[section_index, micro].reshape(N_DP, MB_TOK, MODEL_WIDTH)
            up_seq = upstream[micro].reshape(N_DP, MB_TOK, MODEL_WIDTH)
            loop_carry, dx = lax.scan(one_sequence, loop_carry, (x_seq, up_seq))
            section_inputs.append(dx.reshape(TOKENS, MODEL_WIDTH))
        upstream = jnp.stack(section_inputs)
        all_input.append(upstream)
        dgrads.append(loop_carry)
    all_input = all_input[::-1]
    dgrads = dgrads[::-1]
    input_grad = jnp.stack(all_input)
    outs = [jnp.stack([entry[k] for entry in dgrads]) for k in range(6)]
    return (input_grad, outs[0], outs[1], outs[2], outs[3], outs[4], outs[5])
```

```python
import functools

import jax
import jax.numpy as jnp
import numpy as np
from jax import lax
from jax.experimental import pallas as pl
from jax.experimental.pallas import tpu as pltpu
from jax.sharding import PartitionSpec as P

NOPE = 128
ROPE = 64
VDIM = 128
EPS = 1e-06
SEQ = 64
MESH = pl.DeviceIdType.MESH
F32 = jnp.float32
BF16 = jnp.bfloat16


def rotation_tables(share):
    row = np.arange(2 * SEQ)
    position = (row // (2 * share)) * share + row % share
    lane = np.arange(128)
    freq = np.exp(-np.log(10000.0) * (lane % 32) / 32.0)
    angle = position[:, None] * freq[None, :]
    sign = np.where(lane % 64 < 32, -1.0, 1.0)
    return np.cos(angle).astype(np.float32), (np.sin(angle) * sign).astype(np.float32)


def mm(a, b):
    return jnp.dot(a.astype(BF16), b.astype(BF16), preferred_element_type=F32)


def mm_nt(a, b):
    return lax.dot_general(
        a.astype(BF16), b.astype(BF16), (((1,), (1,)), ((), ())), preferred_element_type=F32
    )


def mm_tn(a, b):
    return lax.dot_general(
        a.astype(BF16), b.astype(BF16), (((0,), (0,)), ((), ())), preferred_element_type=F32
    )


def swap_halves(v):
    lane = lax.broadcasted_iota(jnp.int32, v.shape, 1)
    return jnp.where(lane % 64 < 32, pltpu.roll(v, 96, axis=1), pltpu.roll(v, 32, axis=1))


def kernel(
    sizes,
    x_ref,
    top_ref,
    gain_ref,
    wq_ref,
    wlat_ref,
    cgain_ref,
    wexp_ref,
    wout_ref,
    cos_ref,
    sin_ref,
    dx_out,
    gain_out,
    q_out,
    lat_out,
    lg_out,
    exp_out,
    o_out,
    wg,
    gg,
    xs,
    up,
    part,
    prec,
    dxs,
    rbuf,
    ysend,
    yrecv,
    tot,
    tsend,
    trecv,
    agy_s,
    agy_r,
    ag_s,
    ag_r,
    hop_s,
    hop_r,
    ua_s,
    ua_r,
    tr_s,
    tr_r,
    rs_s,
    rs_r,
    rsy_s,
    rsy_r,
    tg_s,
    tg_r,
):
    sections, nz, nt, width, rank = sizes
    share = SEQ // nt
    rows = 2 * share
    tokens = 2 * SEQ
    cg_at = 512 + rank
    full = cg_at + 128
    pipe = lax.axis_index("pipe")
    dp = lax.axis_index("dp")
    t = lax.axis_index("tensor")
    yl = lax.div(dp, nz)
    z = lax.rem(dp, nz)
    z_right = yl * nz + lax.rem(z + 1, nz)
    z_left = yl * nz + lax.rem(z + nz - 1, nz)
    y_mate = (1 - yl) * nz + z
    others = [k for k in (4, 3, 5, 2, 6, 1, 7) if k < nt]
    arms = (nz // 2, nz - 1 - nz // 2)
    z_to = (z_right, z_left)

    barrier = pltpu.get_barrier_semaphore()

    def greet(where):
        pl.semaphore_signal(barrier, inc=1, device_id=where, device_id_type=MESH)

    greet({"dp": z_right})
    greet({"dp": z_left})
    greet({"dp": y_mate})
    greet({"pipe": lax.rem(pipe + 1, sections)})
    greet({"pipe": lax.rem(pipe + sections - 1, sections)})
    for k in others:
        greet({"tensor": lax.rem(t + k, nt)})

    def block(owner, half=None):
        if half is None:
            return pl.ds(pl.multiple_of(owner * 32, 32), 32)
        return pl.ds(pl.multiple_of(owner * 32 + half * 16, 16), 16)

    own = block(dp)
    wg[own, 0:128] = wout_ref[...].astype(F32).T.astype(BF16)
    wg[block(dp, 0), 128:256] = wexp_ref[:, 0:128]
    wg[block(dp, 1), 128:256] = wexp_ref[:, 128:256]
    wg[own, 256:384] = wq_ref[:, 0:128]
    wg[own, 384:512] = jnp.concatenate(
        [wq_ref[:, 128:192].astype(F32), wlat_ref[:, rank : rank + 64].astype(F32)], axis=1
    ).astype(BF16)
    wg[own, 512:cg_at] = wlat_ref[:, 0:rank]
    lane = lax.broadcasted_iota(jnp.int32, (32, 128), 1)
    line = lax.broadcasted_iota(jnp.int32, (32, 128), 0)
    gain_tile = jnp.concatenate([gain_ref[...].astype(F32)] * 4, axis=1)
    gain_tile = jnp.broadcast_to(gain_tile, (32, 128))
    cgain_tile = jnp.concatenate([cgain_ref[...].astype(F32)] * 8, axis=1)
    cgain_tile = jnp.broadcast_to(cgain_tile, (32, 128))
    placed = jnp.where(
        jnp.logical_and(line == 0, lane // 32 == lax.rem(dp, 4)),
        gain_tile,
        jnp.where(jnp.logical_and(line == 1, lane // 16 == lax.rem(dp, 8)), cgain_tile, 0.0),
    )
    wg[own, cg_at:full] = placed.astype(BF16)

    x32 = x_ref[...].astype(F32)
    for i in range(nt):
        xs[i, 0:share, :] = x32[0, i * share : (i + 1) * share, :]
        xs[i, share:rows, :] = x32[1, i * share : (i + 1) * share, :]

    pl.semaphore_wait(barrier, 5 + len(others))

    def mate_copy(half, owner):
        ref = wg.at[block(owner, half), :]
        return pltpu.make_async_remote_copy(
            ref, ref, agy_s.at[half], agy_r.at[half], device_id={"dp": y_mate}, device_id_type=MESH
        )

    def ring_copy(arm, step, other, half, away):
        shift = step + away
        at = lax.rem(z + nz - shift, nz) if arm == 0 else lax.rem(z + shift, nz)
        line_at = (1 - yl) if other else yl
        ref = wg.at[block(line_at * nz + at, half), :]
        return pltpu.make_async_remote_copy(
            ref,
            ref,
            ag_s.at[arm, step, 2 * other + half],
            ag_r.at[arm, step, 2 * other + half],
            device_id={"dp": z_to[arm]},
            device_id_type=MESH,
        )

    for half in range(2):
        mate_copy(half, dp).start()
        for arm in range(2):
            if arms[arm] > 0:
                ring_copy(arm, 0, 0, half, 0).start()
    for half in range(2):
        mate_copy(half, y_mate).wait_recv()
        for arm in range(2):
            if arms[arm] > 0:
                ring_copy(arm, 0, 1, half, 0).start()
    for step in range(1, arms[0] + 1):
        for other in range(2):
            for half in range(2):
                for arm in range(2):
                    if step <= arms[arm]:
                        ring_copy(arm, step - 1, other, half, 1).wait_recv()
                    if step < arms[arm]:
                        ring_copy(arm, step, other, half, 0).start()

    def gathered_rows(line_at, tiles, per):
        pieces = []
        for tile in range(tiles):
            total = None
            for i in range(per):
                owner = tile * per + i
                value = wg[owner * 32 : owner * 32 + 16, cg_at:full].astype(F32)
                value = value[line_at : line_at + 1, :]
                total = value if total is None else total + value
            pieces.append(total)
        return jnp.concatenate(pieces, axis=1)

    gain = gathered_rows(0, width // 128, 4)
    cgain = gathered_rows(1, rank // 128, 8)
    cosine = cos_ref[...]
    sine = sin_ref[...]

    xf = xs[...].reshape(tokens, width)
    scale_x = lax.rsqrt(jnp.mean(xf * xf, axis=-1, keepdims=True) + EPS)
    rounded = (xf * scale_x * gain).astype(BF16)
    projected = mm(rounded, wg[:, 256:cg_at])
    q_nope = projected[:, 0:128]
    ropes = projected[:, 128:256]
    latent = projected[:, 256:]
    scale_c = lax.rsqrt(jnp.mean(latent * latent, axis=-1, keepdims=True) + EPS)
    latent_hat = latent * scale_c
    compressed = (latent_hat * cgain).astype(BF16)
    ropes = ropes * cosine + swap_halves(ropes) * sine
    wexp = wg[:, 128:256].reshape(2 * nz, 2, 16, 128)
    wexp = jnp.concatenate(
        [wexp[:, 0].reshape(rank, 128), wexp[:, 1].reshape(rank, 128)], axis=1
    )
    expanded = mm(compressed, wexp)
    values = expanded[:, 128:256].astype(BF16)
    lane2 = lax.broadcasted_iota(jnp.int32, (tokens, 128), 1)
    row2 = lax.broadcasted_iota(jnp.int32, (tokens, 128), 0)
    queries = jnp.concatenate([q_nope, jnp.where(lane2 < 64, ropes, 0.0)], axis=1).astype(BF16)
    keys = jnp.concatenate(
        [expanded[:, 0:128], jnp.where(lane2 < 64, pltpu.roll(ropes, 64, axis=1), 0.0)], axis=1
    ).astype(BF16)
    score_scale = (NOPE + ROPE) ** (-0.5)
    scores = mm_nt(queries, keys) * score_scale
    row_position = (row2 // rows) * share + row2 % share
    key_position = (lane2 // rows) * share + lane2 % share
    same = (row2 // share) % 2 == (lane2 // share) % 2
    keep = jnp.logical_and(same, row_position >= key_position)
    scores = jnp.where(keep, scores, -1e30)
    powers = jnp.exp(scores - jnp.max(scores, axis=-1, keepdims=True))
    weights = powers / jnp.sum(powers, axis=-1, keepdims=True)
    weights16 = weights.astype(BF16)
    mixed = mm(weights16, values).astype(BF16)

    def hop_copy(to):
        return pltpu.make_async_remote_copy(
            dxs, up.at[t], hop_s, hop_r, device_id={"pipe": to}, device_id_type=MESH
        )

    def share_copy(k, at):
        ref = up.at[at]
        return pltpu.make_async_remote_copy(
            ref,
            ref,
            ua_s.at[k],
            ua_r.at[k],
            device_id={"tensor": lax.rem(t + k, nt)},
            device_id_type=MESH,
        )

    @pl.when(pipe == sections - 1)
    def _():
        top = top_ref[...].astype(F32)
        for i in range(nt):
            up[i] = jnp.concatenate(
                [top[0, i * share : (i + 1) * share, :], top[1, i * share : (i + 1) * share, :]],
                axis=0,
            ).astype(BF16)

    @pl.when(pipe < sections - 1)
    def _():
        hop_copy(pipe).wait_recv()
        for k in others:
            share_copy(k, t).start()
        for k in others:
            share_copy(k, lax.rem(t + nt - k, nt)).wait_recv()
        for k in others:
            share_copy(k, t).wait_send()

    upstream = up[...].reshape(tokens, width)
    d_mixed = mm(upstream, wg[:, 0:128]).astype(BF16)
    d_weights = mm_nt(d_mixed, values).astype(BF16).astype(F32)
    d_values = mm_tn(weights16, d_mixed).astype(BF16)
    d_scores = weights * (d_weights - jnp.sum(weights * d_weights, axis=-1, keepdims=True))
    d_scores = (d_scores * score_scale).astype(BF16)
    d_queries = mm(d_scores, keys)
    d_keys = mm_tn(d_scores, queries)
    d_ropes = d_queries[:, 128:256] + pltpu.roll(d_keys[:, 128:256], 64, axis=1)
    d_ropes = d_ropes * cosine - swap_halves(d_ropes) * sine
    d_expanded = jnp.concatenate([d_keys[:, 0:128].astype(BF16), d_values], axis=1)
    d_compressed = mm_nt(d_expanded, wexp).astype(BF16).astype(F32)
    d_cgain = jnp.sum(d_compressed * latent_hat, axis=0, keepdims=True)
    d_hat = d_compressed * cgain
    d_latent = scale_c * (d_hat - latent_hat * jnp.mean(d_hat * latent_hat, axis=-1, keepdims=True))
    d_projected = jnp.concatenate(
        [d_queries[:, 0:128].astype(BF16), d_ropes.astype(BF16), d_latent.astype(BF16)], axis=1
    )
    d_rounded = mm_nt(d_projected, wg[:, 256:cg_at]).astype(BF16)
    part[...] = d_rounded.reshape(nt, rows, width)

    def spread_copy(k):
        return pltpu.make_async_remote_copy(
            part.at[lax.rem(t + k, nt)],
            prec.at[k],
            tr_s.at[k],
            tr_r.at[k],
            device_id={"tensor": lax.rem(t + k, nt)},
            device_id_type=MESH,
        )

    for k in others:
        spread_copy(k).start()

    gg[:, 256:cg_at] = mm_tn(rounded, d_projected).astype(BF16)
    gg[:, 0:128] = mm_tn(upstream, mixed).astype(BF16)
    g_exp = mm_tn(compressed, d_expanded).astype(BF16)
    for owner in range(2 * nz):
        gg[owner * 32 : owner * 32 + 16, 128:256] = g_exp[owner * 16 : owner * 16 + 16, 0:128]
        gg[owner * 32 + 16 : owner * 32 + 32, 128:256] = g_exp[
            owner * 16 : owner * 16 + 16, 128:256
        ]

    for k in others:
        spread_copy(k).wait_recv()
    total = part[t].astype(F32)
    for k in others:
        total = total + prec[k].astype(F32)

    x_own = xs[t]
    scale_own = lax.rsqrt(jnp.mean(x_own * x_own, axis=-1, keepdims=True) + EPS)
    hat_own = x_own * scale_own
    d_gain = jnp.sum(total * hat_own, axis=0, keepdims=True)
    d_own = total * gain
    d_x = scale_own * (d_own - hat_own * jnp.mean(d_own * hat_own, axis=-1, keepdims=True))
    d_x = (up[t].astype(F32) + d_x).astype(BF16)
    dxs[...] = d_x

    @pl.when(pipe > 0)
    def _():
        hop_copy(pipe - 1).start()

    d_x32 = d_x.astype(F32)
    dx_out[0] = d_x32[0:share, :].astype(BF16)
    dx_out[1] = d_x32[share:rows, :].astype(BF16)

    for owner in range(2 * nz):
        g_tile = d_gain[:, (owner // 4) * 128 : (owner // 4) * 128 + 128]
        c_tile = d_cgain[:, (owner // 8) * 128 : (owner // 8) * 128 + 128]
        gg[owner * 32 : owner * 32 + 32, cg_at:full] = jnp.where(
            line == 0, g_tile, jnp.where(line == 1, c_tile, 0.0)
        ).astype(BF16)

    def ring_target(arm, step):
        if arm == 0:
            return lax.rem(z + arms[0] - step, nz)
        return lax.rem(z + nz - (arms[1] - step), nz)

    def arrived(arm, step, own_line, half):
        return rbuf.at[arm, step, own_line, half * 16 : half * 16 + 16, :]

    def sum_copy(arm, step, own_line, half):
        if step == 0:
            line_at = yl if own_line else 1 - yl
            source = gg.at[block(line_at * nz + ring_target(arm, 0), half), :]
        else:
            source = arrived(arm, step - 1, own_line, half)
        return pltpu.make_async_remote_copy(
            source,
            arrived(arm, step, own_line, half),
            rs_s.at[arm, step, 2 * own_line + half],
            rs_r.at[arm, step, 2 * own_line + half],
            device_id={"dp": z_to[arm]},
            device_id_type=MESH,
        )

    def y_copy(half):
        return pltpu.make_async_remote_copy(
            ysend.at[half],
            yrecv.at[half],
            rsy_s.at[half],
            rsy_r.at[half],
            device_id={"dp": y_mate},
            device_id_type=MESH,
        )

    for step in range(arms[0] + 1):
        for own_line in range(2):
            line_at = yl if own_line else 1 - yl
            for half in range(2):
                for arm in range(2):
                    if 0 < step <= arms[arm]:
                        sum_copy(arm, step - 1, own_line, half).wait_recv()
                    if 0 < step < arms[arm]:
                        here = block(line_at * nz + ring_target(arm, step), half)
                        held = arrived(arm, step - 1, own_line, half)
                        held[...] = (held[...].astype(F32) + gg[here, :].astype(F32)).astype(BF16)
                    if step < arms[arm]:
                        sum_copy(arm, step, own_line, half).start()
                if step == arms[0]:
                    value = gg[block(line_at * nz + z, half), :].astype(F32)
                    for arm in range(2):
                        if arms[arm] > 0:
                            value = value + arrived(arm, arms[arm] - 1, own_line, half)[...].astype(F32)
                    if own_line:
                        tot[half] = value
                    else:
                        ysend[half] = value.astype(BF16)
                        y_copy(half).start()

    def tensor_copy(k, half):
        return pltpu.make_async_remote_copy(
            tsend.at[half],
            trecv.at[k, half],
            tg_s.at[k, half],
            tg_r.at[k, half],
            device_id={"tensor": lax.rem(t + k, nt)},
            device_id_type=MESH,
        )

    for half in range(2):
        y_copy(half).wait_recv()
        value = tot[half] + yrecv[half].astype(F32)
        tot[half] = value
        tsend[half] = value[:, 384:].astype(BF16)
        for k in others:
            tensor_copy(k, half).start()

    for half in range(2):
        at = half * 16
        value = tot[half]
        o_rows = value[:, 0:128]
        q_out[at : at + 16, 0:128] = value[:, 256:384]
        q_out[at : at + 16, 128:192] = value[:, 384:448]
        exp_out[:, half * 128 : half * 128 + 128] = value[:, 128:256]
        tot[half, :, 0:128] = o_rows
    o_out[...] = jnp.concatenate([tot[0][:, 0:128], tot[1][:, 0:128]], axis=0).T

    for half in range(2):
        at = half * 16
        for k in others:
            tensor_copy(k, half).wait_recv()
        value = tsend[half].astype(F32)
        for k in others:
            value = value + trecv[k, half].astype(F32)
        lat_out[at : at + 16, 0:rank] = value[:, 128 : 128 + rank]
        lat_out[at : at + 16, rank : rank + 64] = value[:, 64:128]
        if half == 0:
            g_row = value[0:1, 128 + rank :]
            c_row = value[1:2, 128 + rank :]
            g_sum = jnp.zeros((1, 32), F32)
            for k in range(4):
                g_sum = g_sum + jnp.where(lax.rem(dp, 4) == k, g_row[:, 32 * k : 32 * k + 32], 0.0)
            c_sum = jnp.zeros((1, 16), F32)
            for k in range(8):
                c_sum = c_sum + jnp.where(lax.rem(dp, 8) == k, c_row[:, 16 * k : 16 * k + 16], 0.0)
            gain_out[...] = g_sum
            lg_out[...] = c_sum

    for half in range(2):
        mate_copy(half, dp).wait_send()
        y_copy(half).wait_send()
        for k in others:
            tensor_copy(k, half).wait_send()
        for other in range(2):
            for arm in range(2):
                for step in range(arms[arm]):
                    ring_copy(arm, step, other, half, 0).wait_send()
                    sum_copy(arm, step, other, half).wait_send()
    for k in others:
        spread_copy(k).wait_send()

    @pl.when(pipe > 0)
    def _():
        hop_copy(pipe - 1).wait_send()


def shards(saved, top_grad, gain, w_query, w_latent, compressed_gain, expand_weight, w_output):
    sections = lax.axis_size("pipe")
    nz = lax.axis_size("dp") // 2
    nt = lax.axis_size("tensor")
    width = saved.shape[3]
    rank = w_latent.shape[2] - ROPE
    share = SEQ // nt
    rows = 2 * share
    full = 640 + rank
    steps = nz // 2
    cosine, sine = rotation_tables(share)
    vmem = pl.BlockSpec(memory_space=pltpu.VMEM)
    dma = pltpu.SemaphoreType.DMA
    outs = pl.pallas_call(
        functools.partial(kernel, (sections, nz, nt, width, rank)),
        out_shape=(
            jax.ShapeDtypeStruct((2, share, width), BF16),
            jax.ShapeDtypeStruct((1, 32), F32),
            jax.ShapeDtypeStruct((32, NOPE + ROPE), F32),
            jax.ShapeDtypeStruct((32, rank + ROPE), F32),
            jax.ShapeDtypeStruct((1, 16), F32),
            jax.ShapeDtypeStruct((16, NOPE + VDIM), F32),
            jax.ShapeDtypeStruct((VDIM, 32), F32),
        ),
        in_specs=[vmem] * 10,
        out_specs=(vmem,) * 7,
        scratch_shapes=[
            pltpu.VMEM((width, full), BF16),
            pltpu.VMEM((width, full), BF16),
            pltpu.VMEM((nt, rows, width), F32),
            pltpu.VMEM((nt, rows, width), BF16),
            pltpu.VMEM((nt, rows, width), BF16),
            pltpu.VMEM((nt, rows, width), BF16),
            pltpu.VMEM((rows, width), BF16),
            pltpu.VMEM((2, steps, 2, 32, full), BF16),
            pltpu.VMEM((2, 16, full), BF16),
            pltpu.VMEM((2, 16, full), BF16),
            pltpu.VMEM((2, 16, full), F32),
            pltpu.VMEM((2, 16, full - 384), BF16),
            pltpu.VMEM((nt, 2, 16, full - 384), BF16),
            dma((2,)),
            dma((2,)),
            dma((2, steps, 4)),
            dma((2, steps, 4)),
            dma,
            dma,
            dma((nt,)),
            dma((nt,)),
            dma((nt,)),
            dma((nt,)),
            dma((2, steps, 4)),
            dma((2, steps, 4)),
            dma((2,)),
            dma((2,)),
            dma((nt, 2)),
            dma((nt, 2)),
        ],
        compiler_params=pltpu.CompilerParams(
            collective_id=0, has_side_effects=True, vmem_limit_bytes=48 * 1024 * 1024
        ),
        name="relay",
    )(
        saved[0],
        top_grad,
        gain,
        w_query[0],
        w_latent[0],
        compressed_gain,
        expand_weight[0],
        w_output[0],
        jnp.asarray(cosine),
        jnp.asarray(sine),
    )
    dx, g_gain, g_q, g_lat, g_lg, g_exp, g_out = outs
    return dx[None], g_gain, g_q[None], g_lat[None], g_lg, g_exp[None], g_out[None]


def solution(mesh):
    in_specs = (
        P("pipe", None, "dp", None),
        P(None, "dp", None),
        P("pipe", "dp"),
        P("pipe", "dp", "tensor"),
        P("pipe", "dp", None),
        P("pipe", "dp"),
        P("pipe", "dp", "tensor"),
        P("pipe", "tensor", "dp"),
    )
    out_specs = (
        P("pipe", None, ("dp", "tensor"), None),
        P("pipe", "dp"),
        P("pipe", "dp", "tensor"),
        P("pipe", "dp", None),
        P("pipe", "dp"),
        P("pipe", "dp", "tensor"),
        P("pipe", "tensor", "dp"),
    )
    return jax.shard_map(shards, mesh=mesh, in_specs=in_specs, out_specs=out_specs, check_vma=False)
```
